256 devices in a mesh: grp: 4 (over y, x), row: 64 (over z, core).
Axes of the slice: x: 2, y: 2, z: 32, core: 2. Of those that a mesh axis runs over, the one named last changes fastest.
The devices are a block of a 4x8x32 slice.
Arguments:
- prior_basis: float32 [262144, 512], P(('grp', 'row')), parts along dimension 0, may hold values from -1 to 1, as said below
- samples: float32 [4, 262144, 64], P(None, ('grp', 'row')), parts along dimension 1, may hold values from -8 to 8
Outputs:
- new_basis: float32 [262144, 256], P(('grp', 'row')), parts along dimension 0
- leaf_estimates: float32 [4, 1024], P(None, ('grp', 'row')), parts along dimension 1
The draws below stay inside these ranges and needn't reach their ends.
There are 4 independent parts, one for each index of `grp`. The reference program is written for one: setup_inputs(seed, part) draws one part's arguments, and reference() takes and returns one part's arrays. A program takes and returns all parts, laid end to end along the dimension named above; each array names one. Nothing has to cross between parts.
Inputs may be any that keep to these rules, and one draw needn't show every extreme that they name: The columns of prior_basis are orthonormal to float32 rounding.
All inputs are finite; a program needn't handle non-finite values.
Results may differ from the reference program's by a relative error of at most 0.0003.
Values sent between devices are 32-bit elements; how exact they have to be, the bound alone decides.
No kernel may reach another device: no remote copies, remote signals or barrier semaphores. Data moves between devices by JAX's collectives and lax.ppermute only.
A program may use at most 64 MiB of HBM per device.

```python
import math
import jax
import jax.numpy as jnp
from jax import lax

ORDER = 65536
BASIS = 512
SAMPLES = 64
LEAF = 256
ROUNDS = 4
LEAVES = 256


def orthonormal_base(key):
    raw_block = jax.random.normal(jax.random.fold_in(key, 11), (ORDER, BASIS), jnp.float32)
    basis_q, upper = jnp.linalg.qr(raw_block)
    return basis_q


def draw_prior_basis(key, part):
    return orthonormal_base(key).astype(jnp.float32)


def draw_samples(key, part):
    basis_q = orthonormal_base(key)
    weights = jax.random.normal(jax.random.fold_in(key, 12), (ROUNDS, BASIS, SAMPLES), jnp.float32)
    weights = weights * jnp.sqrt(ORDER / BASIS)
    low_part = jnp.einsum('nk,rks->rns', basis_q, weights)
    leaf_scale = jnp.exp(jax.random.uniform(jax.random.fold_in(key, 13), (ROUNDS, LEAVES), jnp.float32, math.log(0.05), 0.0))
    row_scale = jnp.repeat(leaf_scale, LEAF, axis=1)[:, :, None]
    noise = jax.random.normal(jax.random.fold_in(key, 14), (ROUNDS, ORDER, SAMPLES), jnp.float32)
    return jnp.clip(low_part + row_scale * noise, -8.0, 8.0).astype(jnp.float32)


def setup_inputs(seed: int = 0, part: int = 0) -> dict:
    splits = jax.random.split(jax.random.key(seed), 3)
    own_keys = jax.random.split(jax.random.fold_in(splits[2], part), 3)
    return {
        "prior_basis": draw_prior_basis(jax.random.fold_in(jax.random.fold_in(splits[2], part), 71), part),
        "samples": draw_samples(jax.random.fold_in(jax.random.fold_in(splits[2], part), 71), part),
    }


def reference(prior_basis, samples):
    highest = lax.Precision.HIGHEST
    new_cols = []
    estimates = []
    for number in range(ROUNDS):
        sample_block = samples[number]
        energy = jnp.sum(sample_block * sample_block)
        c_prior = jnp.dot(prior_basis.T, sample_block, precision=highest)
        remainder = sample_block - jnp.dot(prior_basis, c_prior, precision=highest)
        if new_cols:
            added = jnp.concatenate(new_cols, axis=1)
            c_added = jnp.dot(added.T, sample_block, precision=highest)
            remainder = remainder - jnp.dot(added, c_added, precision=highest)
        gram = jnp.dot(remainder.T, remainder, precision=highest)
        factor = jnp.linalg.cholesky(gram)
        fresh_cols = jax.scipy.linalg.solve_triangular(factor, remainder.T, lower=True).T
        leaf_energy = lax.optimization_barrier(jnp.sum((remainder * remainder).reshape(LEAVES, LEAF, SAMPLES), axis=(1, 2)))
        estimates.append(jnp.sqrt(LEAVES * leaf_energy / energy))
        new_cols.append(fresh_cols)
    return (jnp.concatenate(new_cols, axis=1), jnp.stack(estimates))
```

```python
import functools

import jax
import jax.numpy as jnp
from jax import lax
from jax.experimental import pallas as pl
from jax.experimental.pallas import tpu as pltpu
from jax.sharding import Mesh
from jax.sharding import PartitionSpec as P

LEAF = 256
LANES = 128
NEAR = 4
CORES = 2
ROW = ("far", "near", "core")
GRP_ROW = ("grp",) + ROW
NT = (((1,), (1,)), ((), ()))
TN = (((0,), (0,)), ((), ()))
NN = (((1,), (0,)), ((), ()))


def split(x):
    high = x.astype(jnp.bfloat16)
    low = (x - high.astype(jnp.float32)).astype(jnp.bfloat16)
    return high, low


def dot3(a, b, dims):
    dot = functools.partial(lax.dot_general, dimension_numbers=dims, preferred_element_type=jnp.float32)
    return dot(a[0], b[0]) + (dot(a[0], b[1]) + dot(a[1], b[0]))


def dot_full(a, b, dims):
    return lax.dot_general(a, b, dims, precision=lax.Precision.HIGHEST, preferred_element_type=jnp.float32)


def stats_kernel(core_ref, q_ref, y_ref, mine_ref, theirs_ref, y_out_ref, acc_ref):
    step = pl.program_id(0)
    y = jnp.concatenate([y_ref[r] for r in range(y_ref.shape[0])], axis=1)
    y_out_ref[...] = y
    basis = q_ref.shape[1]
    half = y.shape[1] // CORES
    ys = split(y)
    qs = split(q_ref[...])
    with_basis = dot3(ys, qs, TN)
    with_self = dot3(ys, ys, TN) + lax.dot_general(ys[1], ys[1], TN, preferred_element_type=jnp.float32)

    @pl.when(step == 0)
    def _():
        acc_ref[...] = jnp.zeros_like(acc_ref)

    for c in range(CORES):
        rows = slice(c * half, (c + 1) * half)
        acc_ref[c, :, :basis] += with_basis[rows]
        acc_ref[c, :, basis:] += with_self[rows]

    @pl.when(step == pl.num_programs(0) - 1)
    def _():
        core = core_ref[0]
        for block in range(acc_ref.shape[2] // LANES):
            lanes = slice(block * LANES, (block + 1) * LANES)
            rows = slice(block * half, (block + 1) * half)
            mine_ref[rows, :] = acc_ref[core, :, lanes]
            theirs_ref[rows, :] = acc_ref[1 - core, :, lanes]


def factor_block(block):
    size = block.shape[0]
    row_at = lax.broadcasted_iota(jnp.int32, (size, size), 0)
    lane_at = lax.broadcasted_iota(jnp.int32, (size, size), 1)
    eye = (row_at == lane_at).astype(jnp.float32)
    work = jnp.concatenate([block, eye], axis=1)
    width = 2 * size
    parts = [work[8 * i:8 * i + 8] for i in range(size // 8)]
    sub = lax.broadcasted_iota(jnp.int32, (8, width), 0)
    pivots = []
    for j in range(size):
        at, inner = divmod(j, 8)
        columns = [jnp.broadcast_to(part[:, j:j + 1], (8, width)) for part in parts[at:]]
        pivot = jnp.broadcast_to(columns[0][inner:inner + 1], (8, width))
        row = jnp.broadcast_to(parts[at][inner:inner + 1], (8, width))
        pivots.append(pivot)
        scaled = row * (1.0 / pivot)
        if inner < 7:
            parts[at] = parts[at] - jnp.where(sub > inner, columns[0], 0.0) * scaled
        for i in range(at + 1, len(parts)):
            parts[i] = parts[i] - columns[i - at] * scaled
    scales = []
    for at in range(len(parts)):
        scale = pivots[8 * at]
        for inner in range(1, 8):
            scale = jnp.where(sub == inner, pivots[8 * at + inner], scale)
        scales.append(lax.rsqrt(scale))
    done = jnp.concatenate([part * scale for part, scale in zip(parts, scales)], axis=0)
    upper = jnp.where(row_at <= lane_at, done[:, :size], 0.0)
    return upper, done[:, size:]


def finish_kernel(leaves, sums_ref, q_hbm, y_hbm, v_ref, est_ref, q_ref, y_ref, work_ref, sems):
    q_copy = pltpu.make_async_copy(q_hbm, q_ref, sems.at[0])
    y_copy = pltpu.make_async_copy(y_hbm, y_ref, sems.at[1])
    q_copy.start()
    y_copy.start()
    rows, basis = q_ref.shape
    columns = y_ref.shape[1]
    rounds = est_ref.shape[0]
    size = columns // rounds
    half = columns // CORES

    def lanes_block(block):
        return jnp.concatenate([sums_ref[c, block * half:(block + 1) * half, :] for c in range(CORES)], axis=0)

    coefs = jnp.concatenate([lanes_block(b) for b in range(basis // LANES)], axis=1)
    own = jnp.concatenate([lanes_block(basis // LANES + b) for b in range(columns // LANES)], axis=1)
    row_at = lax.broadcasted_iota(jnp.int32, (columns, columns), 0)
    lane_at = lax.broadcasted_iota(jnp.int32, (columns, columns), 1)
    work_ref[:, :columns] = own - dot_full(coefs, coefs, NT)
    work_ref[:, columns:] = (row_at == lane_at).astype(jnp.float32)
    uppers = []
    for k in range(rounds):
        here = slice(k * size, (k + 1) * size)
        after = slice((k + 1) * size, columns)
        upper, inverse = factor_block(work_ref[here, here])
        uppers.append(upper)
        done = dot_full(inverse, work_ref[here, :], NN)
        work_ref[here, :] = done
        if k + 1 < rounds:
            work_ref[after, :] -= dot_full(done[:, after], done, TN)
    zero = jnp.zeros((size, size), jnp.float32)
    diagonal = jnp.concatenate(
        [jnp.concatenate([uppers[k] if j == k else zero for j in range(rounds)], axis=1) for k in range(rounds)], axis=0
    )
    inverse = work_ref[:, columns:]
    inverse_t = split(jnp.where(row_at >= lane_at, inverse, 0.0))
    diagonal_s = split(diagonal)
    coefs_s = split(coefs)
    q_copy.wait()
    y_copy.wait()
    sums = []
    for leaf in range(rows // LEAF):
        span = slice(leaf * LEAF, (leaf + 1) * LEAF)
        projected = y_ref[span, :] - dot3(split(q_ref[span, :]), coefs_s, NT)
        fresh = dot3(split(projected), inverse_t, NT)
        v_ref[span, :] = fresh
        remainder = dot3(split(fresh), diagonal_s, NN)
        sums.append(jnp.sum(remainder * remainder, axis=0, keepdims=True))
    count = len(sums)
    member = (
        lax.broadcasted_iota(jnp.int32, (8, columns), 0)
        == lax.broadcasted_iota(jnp.int32, (8, columns), 1) // size
    ).astype(jnp.float32)
    leaf_energy = dot_full(member, jnp.concatenate(sums + [jnp.zeros((8 - count, columns), jnp.float32)], axis=0), NT)
    energies = jnp.sum(jnp.where(row_at == lane_at, own, 0.0), axis=0, keepdims=True)
    energy = jnp.sum(member * energies, axis=1, keepdims=True)
    est_ref[...] = jnp.sqrt(leaves * leaf_energy / energy)[:rounds, :count]


def local(prior_basis, samples):
    rounds, rows, size = samples.shape
    basis = prior_basis.shape[1]
    columns = rounds * size
    half = columns // CORES
    depth = (basis + columns) // LANES * half
    far = lax.axis_size("far")
    core = lax.axis_index("core").reshape(1).astype(jnp.int32)
    step = LEAF
    mine, theirs, samples_wide = pl.pallas_call(
        stats_kernel,
        grid=(rows // step,),
        in_specs=[
            pl.BlockSpec(memory_space=pltpu.SMEM),
            pl.BlockSpec((step, basis), lambda i: (i, 0)),
            pl.BlockSpec((rounds, step, size), lambda i: (0, i, 0)),
        ],
        out_specs=[
            pl.BlockSpec((depth, LANES), lambda i: (0, 0)),
            pl.BlockSpec((depth, LANES), lambda i: (0, 0)),
            pl.BlockSpec((step, columns), lambda i: (i, 0)),
        ],
        out_shape=[
            jax.ShapeDtypeStruct((depth, LANES), jnp.float32),
            jax.ShapeDtypeStruct((depth, LANES), jnp.float32),
            jax.ShapeDtypeStruct((rows, columns), jnp.float32),
        ],
        scratch_shapes=[pltpu.VMEM((CORES, half, basis + columns), jnp.float32)],
        name="stats",
    )(core, prior_basis, samples)
    chip = mine + lax.ppermute(theirs, "core", [(0, 1), (1, 0)])
    near_parts = lax.all_to_all(chip.reshape(NEAR, depth // NEAR, LANES), "near", 0, 0, tiled=True)
    near_sum = jnp.sum(near_parts, axis=0).reshape(far, depth // NEAR // far, LANES)
    far_parts = lax.all_to_all(near_sum, "far", 0, 0, tiled=True)
    total = jnp.sum(far_parts, axis=0)
    far_all = lax.all_to_all(jnp.broadcast_to(total, far_parts.shape), "far", 0, 0, tiled=True)
    sums = lax.all_gather(far_all.reshape(1, depth // NEAR, LANES), ("core", "near"), axis=0, tiled=True)
    sums = sums.reshape(CORES, depth, LANES)
    leaves = rows // LEAF * far * NEAR * CORES
    return pl.pallas_call(
        functools.partial(finish_kernel, float(leaves)),
        in_specs=[
            pl.BlockSpec(memory_space=pltpu.VMEM),
            pl.BlockSpec(memory_space=pl.ANY),
            pl.BlockSpec(memory_space=pl.ANY),
        ],
        out_specs=[pl.BlockSpec(memory_space=pltpu.VMEM), pl.BlockSpec(memory_space=pltpu.VMEM)],
        out_shape=[
            jax.ShapeDtypeStruct((rows, columns), jnp.float32),
            jax.ShapeDtypeStruct((rounds, rows // LEAF), jnp.float32),
        ],
        scratch_shapes=[
            pltpu.VMEM((rows, basis), jnp.float32),
            pltpu.VMEM((rows, columns), jnp.float32),
            pltpu.VMEM((columns, 2 * columns), jnp.float32),
            pltpu.SemaphoreType.DMA((2,)),
        ],
        name="finish",
    )(sums, prior_basis, samples_wide)


def solution(mesh):
    grp = mesh.shape["grp"]
    far = mesh.shape["row"] // (NEAR * CORES)
    parts = Mesh(mesh.devices.reshape(grp, far, NEAR, CORES), GRP_ROW)
    in_specs = (P(GRP_ROW, None), P(None, GRP_ROW, None))
    out_specs = (P(GRP_ROW, None), P(None, GRP_ROW))
    return jax.shard_map(local, mesh=parts, in_specs=in_specs, out_specs=out_specs, check_vma=False)
```

```python
import functools
import math

import jax
import jax.numpy as jnp
from jax import lax
from jax.experimental import pallas as pl
from jax.experimental.pallas import tpu as pltpu
from jax.sharding import Mesh
from jax.sharding import PartitionSpec as P

LEAF = 256
LANES = 128
NEAR = 4
CORES = 2
ROW = ("far", "near", "core")
GRP_ROW = ("grp",) + ROW
NT = (((1,), (1,)), ((), ()))
TN = (((0,), (0,)), ((), ()))
NN = (((1,), (0,)), ((), ()))


def split(x):
    high = x.astype(jnp.bfloat16)
    low = (x - high.astype(jnp.float32)).astype(jnp.bfloat16)
    return high, low


def dot3(a, b, dims):
    dot = functools.partial(lax.dot_general, dimension_numbers=dims, preferred_element_type=jnp.float32)
    return dot(a[0], b[0]) + (dot(a[0], b[1]) + dot(a[1], b[0]))


def dot_full(a, b, dims):
    return lax.dot_general(a, b, dims, precision=lax.Precision.HIGHEST, preferred_element_type=jnp.float32)


def stats_kernel(core_ref, q_ref, yt_ref, mine_ref, theirs_ref, acc_ref):
    step = pl.program_id(0)
    yt = yt_ref[...].reshape(-1, yt_ref.shape[2])
    basis = q_ref.shape[1]
    half = yt.shape[0] // CORES
    ys = split(yt)
    with_basis = dot3(ys, split(q_ref[...]), NN)
    with_self = dot3(ys, ys, NT) + lax.dot_general(ys[1], ys[1], NT, preferred_element_type=jnp.float32)

    @pl.when(step == 0)
    def _():
        acc_ref[...] = jnp.zeros_like(acc_ref)

    for c in range(CORES):
        rows = slice(c * half, (c + 1) * half)
        acc_ref[c, :, :basis] += with_basis[rows]
        acc_ref[c, :, basis:] += with_self[rows]

    @pl.when(step == pl.num_programs(0) - 1)
    def _():
        core = core_ref[0]
        for block in range(acc_ref.shape[2] // LANES):
            lanes = slice(block * LANES, (block + 1) * LANES)
            rows = slice(block * half, (block + 1) * half)
            mine_ref[rows, :] = acc_ref[core, :, lanes]
            theirs_ref[rows, :] = acc_ref[1 - core, :, lanes]


def spread_row(x, r):
    return jnp.broadcast_to(x[r:r + 1], x.shape)


def factor_block(block):
    size = block.shape[0]
    row_at = lax.broadcasted_iota(jnp.int32, (size, size), 0)
    lane_at = lax.broadcasted_iota(jnp.int32, (size, size), 1)
    eye = (row_at == lane_at).astype(jnp.float32)
    work = jnp.concatenate([block, eye], axis=1)
    width = 2 * size
    count = size // 8
    parts = [work[8 * i:8 * i + 8] for i in range(count)]
    sub = lax.broadcasted_iota(jnp.int32, (8, width), 0)
    done = []
    for p in range(count):
        cols = [
            [jnp.take_along_axis(parts[i], jnp.full((8, width), 8 * p + m, jnp.int32), axis=1) for m in range(8)]
            for i in range(p, count)
        ]
        own = cols[0]
        pivots = None
        steps = []
        for m in range(8):
            pivot = spread_row(own[m], m)
            pivots = pivot if m == 0 else jnp.where(sub == m, pivot, pivots)
            inverse = 1.0 / pivot
            row = spread_row(parts[p], m) * inverse
            entries = {k: spread_row(own[k], m) * inverse for k in range(m + 1, 8)}
            steps.append((row, entries))
            if m < 7:
                below = jnp.where(sub > m, own[m], 0.0)
                for k in range(m + 1, 8):
                    own[k] = own[k] - below * entries[k]
                parts[p] = parts[p] - below * row
        done.append(parts[p] * lax.rsqrt(pivots))
        for i in range(p + 1, count):
            col = cols[i - p]
            for m, (row, entries) in enumerate(steps):
                parts[i] = parts[i] - col[m] * row
                for k in range(m + 1, 8):
                    col[k] = col[k] - col[m] * entries[k]
    done = jnp.concatenate(done, axis=0)
    upper = jnp.where(row_at <= lane_at, done[:, :size], 0.0)
    return upper, done[:, size:]


def finish_kernel(leaves, sums_ref, q_hbm, yt_hbm, v_ref, est_ref, q_ref, yt_ref, work_ref, sems):
    q_copy = pltpu.make_async_copy(q_hbm, q_ref, sems.at[0])
    y_copy = pltpu.make_async_copy(yt_hbm, yt_ref, sems.at[1])
    q_copy.start()
    y_copy.start()
    rows, basis = q_ref.shape
    columns = yt_ref.shape[0] * yt_ref.shape[1]
    rounds = est_ref.shape[0]
    size = columns // rounds
    half = columns // CORES

    unit_rows = math.gcd(half, sums_ref.shape[2])
    units_near = sums_ref.shape[2] // unit_rows

    def lanes_block(block):
        units = [divmod(unit, units_near) for unit in range(block * half // unit_rows, (block + 1) * half // unit_rows)]
        return jnp.concatenate(
            [
                sums_ref[near, c, part * unit_rows:(part + 1) * unit_rows, :]
                for c in range(CORES)
                for near, part in units
            ],
            axis=0,
        )

    coefs = jnp.concatenate([lanes_block(b) for b in range(basis // LANES)], axis=1)
    own = jnp.concatenate([lanes_block(basis // LANES + b) for b in range(columns // LANES)], axis=1)
    row_at = lax.broadcasted_iota(jnp.int32, (columns, columns), 0)
    lane_at = lax.broadcasted_iota(jnp.int32, (columns, columns), 1)
    work_ref[:, :columns] = own - dot_full(coefs, coefs, NT)
    work_ref[:, columns:] = (row_at == lane_at).astype(jnp.float32)
    uppers = []
    for k in range(rounds):
        here = slice(k * size, (k + 1) * size)
        after = slice((k + 1) * size, columns)
        upper, inverse = factor_block(work_ref[here, here])
        uppers.append(upper)
        done = dot_full(inverse, work_ref[here, :], NN)
        work_ref[here, :] = done
        if k + 1 < rounds:
            work_ref[after, :] -= dot_full(done[:, after], done, TN)
    zero = jnp.zeros((size, size), jnp.float32)
    diagonal = jnp.concatenate(
        [jnp.concatenate([uppers[k] if j == k else zero for j in range(rounds)], axis=1) for k in range(rounds)], axis=0
    )
    inverse = work_ref[:, columns:]
    inverse_t = split(jnp.where(row_at >= lane_at, inverse, 0.0))
    diagonal_s = split(diagonal)
    coefs_s = split(coefs)
    q_copy.wait()
    y_copy.wait()
    sums = []
    for leaf in range(rows // LEAF):
        span = slice(leaf * LEAF, (leaf + 1) * LEAF)
        samples = yt_ref[:, :, span].reshape(columns, LEAF).T
        projected = samples - dot3(split(q_ref[span, :]), coefs_s, NT)
        fresh = dot3(split(projected), inverse_t, NT)
        v_ref[span, :] = fresh
        remainder = dot3(split(fresh), diagonal_s, NN)
        sums.append(jnp.sum(remainder * remainder, axis=0, keepdims=True))
    count = len(sums)
    member = (
        lax.broadcasted_iota(jnp.int32, (8, columns), 0)
        == lax.broadcasted_iota(jnp.int32, (8, columns), 1) // size
    ).astype(jnp.float32)
    leaf_energy = dot_full(member, jnp.concatenate(sums + [jnp.zeros((8 - count, columns), jnp.float32)], axis=0), NT)
    energies = jnp.sum(jnp.where(row_at == lane_at, own, 0.0), axis=0, keepdims=True)
    energy = jnp.sum(member * energies, axis=1, keepdims=True)
    est_ref[...] = jnp.sqrt(leaves * leaf_energy / energy)[:rounds, :count]


def local(prior_basis, samples):
    rounds, rows, size = samples.shape
    basis = prior_basis.shape[1]
    columns = rounds * size
    half = columns // CORES
    depth = (basis + columns) // LANES * half
    far = lax.axis_size("far")
    core = lax.axis_index("core").reshape(1).astype(jnp.int32)
    step = LEAF
    samples_t = jnp.transpose(samples, (0, 2, 1))
    mine, theirs = pl.pallas_call(
        stats_kernel,
        grid=(rows // step,),
        in_specs=[
            pl.BlockSpec(memory_space=pltpu.SMEM),
            pl.BlockSpec((step, basis), lambda i: (i, 0)),
            pl.BlockSpec((rounds, size, step), lambda i: (0, 0, i)),
        ],
        out_specs=[
            pl.BlockSpec((depth, LANES), lambda i: (0, 0)),
            pl.BlockSpec((depth, LANES), lambda i: (0, 0)),
        ],
        out_shape=[
            jax.ShapeDtypeStruct((depth, LANES), jnp.float32),
            jax.ShapeDtypeStruct((depth, LANES), jnp.float32),
        ],
        scratch_shapes=[pltpu.VMEM((CORES, half, basis + columns), jnp.float32)],
        name="stats",
    )(core, prior_basis, samples_t)
    chip = mine + lax.ppermute(theirs, "core", [(0, 1), (1, 0)])
    near_parts = lax.all_to_all(chip.reshape(NEAR, depth // NEAR, LANES), "near", 0, 0, tiled=True)
    near_sum = jnp.sum(near_parts, axis=0).reshape(far, depth // NEAR // far, LANES)
    far_parts = lax.all_to_all(near_sum, "far", 0, 0, tiled=True)
    total = jnp.sum(far_parts, axis=0)
    far_all = lax.all_to_all(jnp.broadcast_to(total, far_parts.shape), "far", 0, 0, tiled=True)
    sums = lax.all_gather(far_all.reshape(1, depth // NEAR, LANES), ("near", "core"), axis=0, tiled=True)
    sums = sums.reshape(NEAR, CORES, depth // NEAR, LANES)
    leaves = rows // LEAF * far * NEAR * CORES
    return pl.pallas_call(
        functools.partial(finish_kernel, float(leaves)),
        in_specs=[
            pl.BlockSpec(memory_space=pltpu.VMEM),
            pl.BlockSpec(memory_space=pl.ANY),
            pl.BlockSpec(memory_space=pl.ANY),
        ],
        out_specs=[pl.BlockSpec(memory_space=pltpu.VMEM), pl.BlockSpec(memory_space=pltpu.VMEM)],
        out_shape=[
            jax.ShapeDtypeStruct((rows, columns), jnp.float32),
            jax.ShapeDtypeStruct((rounds, rows // LEAF), jnp.float32),
        ],
        scratch_shapes=[
            pltpu.VMEM((rows, basis), jnp.float32),
            pltpu.VMEM((rounds, size, rows), jnp.float32),
            pltpu.VMEM((columns, 2 * columns), jnp.float32),
            pltpu.SemaphoreType.DMA((2,)),
        ],
        name="finish",
    )(sums, prior_basis, samples_t)


def solution(mesh):
    grp = mesh.shape["grp"]
    far = mesh.shape["row"] // (NEAR * CORES)
    parts = Mesh(mesh.devices.reshape(grp, far, NEAR, CORES), GRP_ROW)
    in_specs = (P(GRP_ROW, None), P(None, GRP_ROW, None))
    out_specs = (P(GRP_ROW, None), P(None, GRP_ROW))
    return jax.shard_map(local, mesh=parts, in_specs=in_specs, out_specs=out_specs, check_vma=False)
```

```python
import functools

import jax
import jax.numpy as jnp
from jax import lax
from jax.experimental import pallas as pl
from jax.experimental.pallas import tpu as pltpu
from jax.sharding import Mesh
from jax.sharding import PartitionSpec as P

LEAF = 256
LANES = 128
NEAR = 4
CORES = 2
PIECES = 5
ROW = ("far", "near", "core")
GRP_ROW = ("grp",) + ROW
CHIP = ("far", "near")
SWAP = [(0, 1), (1, 0)]
NT = (((1,), (1,)), ((), ()))
TN = (((0,), (0,)), ((), ()))
NN = (((1,), (0,)), ((), ()))


def split(x):
    high = x.astype(jnp.bfloat16)
    low = (x - high.astype(jnp.float32)).astype(jnp.bfloat16)
    return high, low


def dot3(a, b, dims):
    dot = functools.partial(lax.dot_general, dimension_numbers=dims, preferred_element_type=jnp.float32)
    return dot(a[0], b[0]) + (dot(a[0], b[1]) + dot(a[1], b[0]))


def dot_full(a, b, dims):
    return lax.dot_general(a, b, dims, precision=lax.Precision.HIGHEST, preferred_element_type=jnp.float32)


def stats_kernel(core_ref, near_ref, q_ref, yt_ref, mine_ref, theirs_ref, acc_ref):
    step = pl.program_id(0)
    yt = yt_ref[...].reshape(-1, yt_ref.shape[2])
    basis = q_ref.shape[1]
    half = yt.shape[0] // CORES
    quarter = acc_ref.shape[1] // NEAR
    ys = split(yt)
    with_basis = dot3(ys, split(q_ref[...]), NN)
    with_self = dot3(ys, ys, NT) + lax.dot_general(ys[1], ys[1], NT, preferred_element_type=jnp.float32)

    @pl.when(step == 0)
    def _():
        acc_ref[...] = jnp.zeros_like(acc_ref)

    for c in range(CORES):
        rows = slice(c * half, (c + 1) * half)
        for product, base in ((with_basis, 0), (with_self, basis // LANES)):
            for block in range(product.shape[1] // LANES):
                at = (base + block) * half
                acc_ref[c, at:at + half, :] += product[rows, block * LANES:(block + 1) * LANES]

    @pl.when(step == pl.num_programs(0) - 1)
    def _():
        core = core_ref[0]
        for slot in range(NEAR):
            source = pl.multiple_of(lax.rem(near_ref[0] + slot, NEAR) * quarter, 8)
            rows = slice(slot * quarter, (slot + 1) * quarter)
            mine_ref[rows, :] = acc_ref[core, pl.ds(source, quarter), :]
            theirs_ref[rows, :] = acc_ref[1 - core, pl.ds(source, quarter), :]


def piece_rows(quarter):
    return ((0, 0, quarter), (1, 0, quarter), (3, 0, quarter), (2, 0, quarter // 2), (2, quarter // 2, quarter // 2))


def spread_row(x, r):
    return jnp.broadcast_to(x[r:r + 1], x.shape)


def factor_block(block, panel=16):
    size = block.shape[0]
    row_at = lax.broadcasted_iota(jnp.int32, (size, size), 0)
    lane_at = lax.broadcasted_iota(jnp.int32, (size, size), 1)
    eye = (row_at == lane_at).astype(jnp.float32)
    work = jnp.concatenate([block, eye], axis=1)
    width = 2 * size
    count = size // 8
    high = panel // 8
    parts = [work[8 * i:8 * i + 8] for i in range(count)]
    sub = lax.broadcasted_iota(jnp.int32, (8, width), 0)
    done = []
    for p in range(0, count, high):
        cols = {
            i: [jnp.take_along_axis(parts[i], jnp.full((8, width), 8 * p + m, jnp.int32), axis=1) for m in range(panel)]
            for i in range(p, count)
        }
        steps = []
        for q in range(p, p + high):
            pivots = None
            for r in range(8):
                m = 8 * (q - p) + r
                pivot = spread_row(cols[q][m], r)
                pivots = pivot if r == 0 else jnp.where(sub == r, pivot, pivots)
                inverse = 1.0 / pivot
                row = spread_row(parts[q], r)
                heads = {k: spread_row(cols[q][k], r) for k in range(m + 1, panel)}
                for i in range(q, p + high):
                    col = jnp.where(sub > r, cols[i][m], 0.0) if i == q else cols[i][m]
                    for k in range(m + 1, panel):
                        cols[i][k] = cols[i][k] - (col * heads[k]) * inverse
                    parts[i] = parts[i] - (col * row) * inverse
                steps.append((row * inverse, {k: heads[k] * inverse for k in heads}))
            done.append(parts[q] * lax.rsqrt(pivots))
        for i in range(p + high, count):
            col = cols[i]
            for m, (row, entries) in enumerate(steps):
                parts[i] = parts[i] - col[m] * row
                for k in range(m + 1, panel):
                    col[k] = col[k] - col[m] * entries[k]
    done = jnp.concatenate(done, axis=0)
    upper = jnp.where(row_at <= lane_at, done[:, :size], 0.0)
    return upper, done[:, size:]


def finish_kernel(leaves, core_ref, near_ref, *refs):
    parts = refs[:CORES * PIECES]
    q_hbm, yt_hbm, v_ref, est_ref, q_ref, yt_ref, work_ref, p_ref, sums_ref, sems = refs[CORES * PIECES:]
    q_copy = pltpu.make_async_copy(q_hbm, q_ref, sems.at[0])
    y_copy = pltpu.make_async_copy(yt_hbm, yt_ref, sems.at[1])
    q_copy.start()
    y_copy.start()
    rows, basis = q_ref.shape
    columns = yt_ref.shape[0] * yt_ref.shape[1]
    rounds = est_ref.shape[0]
    size = columns // rounds
    half = columns // CORES

    quarter = sums_ref.shape[1] // NEAR
    core, near = core_ref[0], near_ref[0]
    for side in range(CORES):
        half_at = core if side == 0 else 1 - core
        for piece, (slot, first, size_at) in enumerate(piece_rows(quarter)):
            at = pl.multiple_of(lax.rem(near + slot, NEAR) * quarter + first, 8)
            sums_ref[half_at, pl.ds(at, size_at), :] = parts[side * PIECES + piece][...]

    def lanes_block(block):
        return jnp.concatenate([sums_ref[c, block * half:(block + 1) * half, :] for c in range(CORES)], axis=0)

    coefs = jnp.concatenate([lanes_block(b) for b in range(basis // LANES)], axis=1)
    own = jnp.concatenate([lanes_block(basis // LANES + b) for b in range(columns // LANES)], axis=1)
    row_at = lax.broadcasted_iota(jnp.int32, (columns, columns), 0)
    lane_at = lax.broadcasted_iota(jnp.int32, (columns, columns), 1)
    work_ref[:, :columns] = own - dot_full(coefs, coefs, NT)
    work_ref[:, columns:] = (row_at == lane_at).astype(jnp.float32)
    coefs_s = split(coefs)
    leaf_count = rows // LEAF

    def project(leaf):
        span = slice(leaf * LEAF, (leaf + 1) * LEAF)
        block = yt_ref[:, :, span].reshape(columns, LEAF).T
        p_ref[span, :] = block - dot3(split(q_ref[span, :]), coefs_s, NT)

    uppers = []
    for k in range(rounds):
        here = slice(k * size, (k + 1) * size)
        after = slice((k + 1) * size, columns)
        if k > 0:
            for leaf in range((k - 1) * leaf_count // (rounds - 1), k * leaf_count // (rounds - 1)):
                project(leaf)
        upper, inverse = factor_block(work_ref[here, here])
        uppers.append(upper)
        done = dot_full(inverse, work_ref[here, :], NN)
        work_ref[here, :] = done
        if k + 1 < rounds:
            work_ref[after, :] -= dot_full(done[:, after], done, TN)
        if k == 0:
            q_copy.wait()
            y_copy.wait()
    zero = jnp.zeros((size, size), jnp.float32)
    diagonal = jnp.concatenate(
        [jnp.concatenate([uppers[k] if j == k else zero for j in range(rounds)], axis=1) for k in range(rounds)], axis=0
    )
    inverse = work_ref[:, columns:]
    inverse_t = split(jnp.where(row_at >= lane_at, inverse, 0.0))
    diagonal_s = split(diagonal)
    sums = []
    for leaf in range(leaf_count):
        span = slice(leaf * LEAF, (leaf + 1) * LEAF)
        fresh = dot3(split(p_ref[span, :]), inverse_t, NT)
        v_ref[span, :] = fresh
        remainder = dot3(split(fresh), diagonal_s, NN)
        sums.append(jnp.sum(remainder * remainder, axis=0, keepdims=True))
    count = len(sums)
    member = (
        lax.broadcasted_iota(jnp.int32, (8, columns), 0)
        == lax.broadcasted_iota(jnp.int32, (8, columns), 1) // size
    ).astype(jnp.float32)
    leaf_energy = dot_full(member, jnp.concatenate(sums + [jnp.zeros((8 - count, columns), jnp.float32)], axis=0), NT)
    energies = jnp.sum(jnp.where(row_at == lane_at, own, 0.0), axis=0, keepdims=True)
    energy = jnp.sum(member * energies, axis=1, keepdims=True)
    est_ref[...] = jnp.sqrt(leaves * leaf_energy / energy)[:rounds, :count]


def run_finish(leaves, core, near, parts, prior_basis, samples_t):
    rows, basis = prior_basis.shape
    rounds, size, _ = samples_t.shape
    columns = rounds * size
    depth = (basis + columns) // LANES * (columns // CORES)
    whole = pl.BlockSpec(memory_space=pltpu.VMEM)
    return pl.pallas_call(
        functools.partial(finish_kernel, leaves),
        in_specs=[pl.BlockSpec(memory_space=pltpu.SMEM)] * 2
        + [whole] * len(parts)
        + [pl.BlockSpec(memory_space=pl.ANY), pl.BlockSpec(memory_space=pl.ANY)],
        out_specs=[whole, whole],
        out_shape=[
            jax.ShapeDtypeStruct((rows, columns), jnp.float32),
            jax.ShapeDtypeStruct((rounds, rows // LEAF), jnp.float32),
        ],
        scratch_shapes=[
            pltpu.VMEM((rows, basis), jnp.float32),
            pltpu.VMEM((rounds, size, rows), jnp.float32),
            pltpu.VMEM((columns, 2 * columns), jnp.float32),
            pltpu.VMEM((rows, columns), jnp.float32),
            pltpu.VMEM((CORES, depth, LANES), jnp.float32),
            pltpu.SemaphoreType.DMA((2,)),
        ],
        name="finish",
    )(core, near, *parts, prior_basis, samples_t)


def shifted(x, hops):
    count = lax.axis_size(CHIP)
    return lax.ppermute(x, CHIP, [(i, (i + hops) % count) for i in range(count)])


def local(prior_basis, samples):
    rounds, rows, size = samples.shape
    basis = prior_basis.shape[1]
    columns = rounds * size
    half = columns // CORES
    depth = (basis + columns) // LANES * half
    quarter = depth // NEAR
    far = lax.axis_size("far")
    core = lax.axis_index("core").reshape(1).astype(jnp.int32)
    near = lax.axis_index("near").reshape(1).astype(jnp.int32)
    step = LEAF
    samples_t = jnp.transpose(samples, (0, 2, 1))
    mine, theirs = pl.pallas_call(
        stats_kernel,
        grid=(rows // step,),
        in_specs=[
            pl.BlockSpec(memory_space=pltpu.SMEM),
            pl.BlockSpec(memory_space=pltpu.SMEM),
            pl.BlockSpec((step, basis), lambda i: (i, 0)),
            pl.BlockSpec((rounds, size, step), lambda i: (0, 0, i)),
        ],
        out_specs=[
            pl.BlockSpec((depth, LANES), lambda i: (0, 0)),
            pl.BlockSpec((depth, LANES), lambda i: (0, 0)),
        ],
        out_shape=[
            jax.ShapeDtypeStruct((depth, LANES), jnp.float32),
            jax.ShapeDtypeStruct((depth, LANES), jnp.float32),
        ],
        scratch_shapes=[pltpu.VMEM((CORES, depth, LANES), jnp.float32)],
        name="stats",
    )(core, near, prior_basis, samples_t)
    chip = (mine + lax.ppermute(theirs, "core", SWAP)).reshape(NEAR, quarter, LANES)
    middle = quarter // 2
    from_left = shifted(chip[1], 1)
    from_right = shifted(chip[3], -1)
    from_far_left = shifted(chip[2, :middle], 2)
    from_far_right = shifted(chip[2, middle:], -2)
    near_sum = chip[0] + from_left + from_right + jnp.concatenate([from_far_left, from_far_right], axis=0)
    far_parts = lax.all_to_all(near_sum.reshape(far, quarter // far, LANES), "far", 0, 0, tiled=True)
    total = jnp.sum(far_parts, axis=0)
    own = lax.all_to_all(jnp.broadcast_to(total, far_parts.shape), "far", 0, 0, tiled=True).reshape(quarter, LANES)
    pieces = [own, shifted(own, -1), shifted(own, 1), shifted(own[:middle], 2), shifted(own[middle:], -2)]
    parts = pieces + [lax.ppermute(piece, "core", SWAP) for piece in pieces]
    leaves = float(rows // LEAF * far * NEAR * CORES)
    return run_finish(leaves, core, near, parts, prior_basis, samples_t)


def solution(mesh):
    grp = mesh.shape["grp"]
    far = mesh.shape["row"] // (NEAR * CORES)
    parts = Mesh(mesh.devices.reshape(grp, far, NEAR, CORES), GRP_ROW)
    in_specs = (P(GRP_ROW, None), P(None, GRP_ROW, None))
    out_specs = (P(GRP_ROW, None), P(None, GRP_ROW))
    return jax.shard_map(local, mesh=parts, in_specs=in_specs, out_specs=out_specs, check_vma=False)
```

```python
import functools

import jax
import jax.numpy as jnp
from jax import lax
from jax.experimental import pallas as pl
from jax.experimental.pallas import tpu as pltpu
from jax.sharding import Mesh
from jax.sharding import PartitionSpec as P

LEAF = 256
LANES = 128
NEAR = 4
CORES = 2
PIECES = 5
ROW = ("far", "near", "core")
GRP_ROW = ("grp",) + ROW
CHIP = ("far", "near")
SWAP = [(0, 1), (1, 0)]
NT = (((1,), (1,)), ((), ()))
TN = (((0,), (0,)), ((), ()))
NN = (((1,), (0,)), ((), ()))


def split(x):
    high = x.astype(jnp.bfloat16)
    low = (x - high.astype(jnp.float32)).astype(jnp.bfloat16)
    return high, low


def dot_parts(a, b, dims, pairs):
    ((lhs_at,), (rhs_at,)), _ = dims
    lhs = jnp.concatenate([a[i] for i, _ in pairs], axis=lhs_at)
    rhs = jnp.concatenate([b[j] for _, j in pairs], axis=rhs_at)
    return lax.dot_general(lhs, rhs, dims, preferred_element_type=jnp.float32)


def dot3(a, b, dims):
    return dot_parts(a, b, dims, ((0, 0), (0, 1), (1, 0)))


def dot4(a, b, dims):
    return dot_parts(a, b, dims, ((0, 0), (0, 1), (1, 0), (1, 1)))


def stats_kernel(core_ref, near_ref, q_ref, yt_ref, mine_ref, theirs_ref, acc_ref):
    step = pl.program_id(0)
    yt = yt_ref[...].reshape(-1, yt_ref.shape[2])
    basis = q_ref.shape[1]
    half = yt.shape[0] // CORES
    quarter = acc_ref.shape[1] // NEAR
    ys = split(yt)
    with_basis = dot3(ys, split(q_ref[...]), NN)
    with_self = dot4(ys, ys, NT)

    @pl.when(step == 0)
    def _():
        acc_ref[...] = jnp.zeros_like(acc_ref)

    for c in range(CORES):
        rows = slice(c * half, (c + 1) * half)
        for product, base in ((with_basis, 0), (with_self, basis // LANES)):
            for block in range(product.shape[1] // LANES):
                at = (base + block) * half
                acc_ref[c, at:at + half, :] += product[rows, block * LANES:(block + 1) * LANES]

    @pl.when(step == pl.num_programs(0) - 1)
    def _():
        core = core_ref[0]
        for slot in range(NEAR):
            source = pl.multiple_of(lax.rem(near_ref[0] + slot, NEAR) * quarter, 8)
            rows = slice(slot * quarter, (slot + 1) * quarter)
            mine_ref[rows, :] = acc_ref[core, pl.ds(source, quarter), :]
            theirs_ref[rows, :] = acc_ref[1 - core, pl.ds(source, quarter), :]


def piece_rows(quarter):
    return ((0, 0, quarter), (1, 0, quarter), (3, 0, quarter), (2, 0, quarter // 2), (2, quarter // 2, quarter // 2))


def spread_row(x, r):
    return jnp.broadcast_to(x[r:r + 1], x.shape)


def factor_block(block, panel=16):
    size = block.shape[0]
    row_at = lax.broadcasted_iota(jnp.int32, (size, size), 0)
    lane_at = lax.broadcasted_iota(jnp.int32, (size, size), 1)
    eye = (row_at == lane_at).astype(jnp.float32)
    work = jnp.concatenate([block, eye], axis=1)
    width = 2 * size
    count = size // 8
    high = panel // 8
    parts = [work[8 * i:8 * i + 8] for i in range(count)]
    sub = lax.broadcasted_iota(jnp.int32, (8, width), 0)
    done = []
    for p in range(0, count, high):
        cols = {
            i: [jnp.take_along_axis(parts[i], jnp.full((8, width), 8 * p + m, jnp.int32), axis=1) for m in range(panel)]
            for i in range(p, count)
        }
        steps = []
        for q in range(p, p + high):
            pivots = None
            for r in range(8):
                m = 8 * (q - p) + r
                pivot = spread_row(cols[q][m], r)
                pivots = pivot if r == 0 else jnp.where(sub == r, pivot, pivots)
                inverse = 1.0 / pivot
                row = spread_row(parts[q], r)
                heads = {k: spread_row(cols[q][k], r) for k in range(m + 1, panel)}
                for i in range(q, p + high):
                    col = jnp.where(sub > r, cols[i][m], 0.0) if i == q else cols[i][m]
                    for k in range(m + 1, panel):
                        cols[i][k] = cols[i][k] - (col * heads[k]) * inverse
                    parts[i] = parts[i] - (col * row) * inverse
                steps.append((row * inverse, {k: heads[k] * inverse for k in heads}))
            done.append(parts[q] * lax.rsqrt(pivots))
        for i in range(p + high, count):
            col = cols[i]
            for m, (row, entries) in enumerate(steps):
                parts[i] = parts[i] - col[m] * row
                for k in range(m + 1, panel):
                    col[k] = col[k] - col[m] * entries[k]
    done = jnp.concatenate(done, axis=0)
    upper = jnp.where(row_at <= lane_at, done[:, :size], 0.0)
    return upper, done[:, size:]


def finish_kernel(leaves, core_ref, near_ref, *refs):
    parts = refs[:CORES * PIECES]
    q_hbm, yt_hbm, v_ref, est_ref, q_ref, yt_ref, work_ref, p_ref, sums_ref, sems = refs[CORES * PIECES:]
    q_copy = pltpu.make_async_copy(q_hbm, q_ref, sems.at[0])
    y_copy = pltpu.make_async_copy(yt_hbm, yt_ref, sems.at[1])
    q_copy.start()
    y_copy.start()
    rows, basis = q_ref.shape
    columns = yt_ref.shape[0] * yt_ref.shape[1]
    rounds = est_ref.shape[0]
    size = columns // rounds
    half = columns // CORES

    quarter = sums_ref.shape[1] // NEAR
    core, near = core_ref[0], near_ref[0]
    for side in range(CORES):
        half_at = core if side == 0 else 1 - core
        for piece, (slot, first, size_at) in enumerate(piece_rows(quarter)):
            at = pl.multiple_of(lax.rem(near + slot, NEAR) * quarter + first, 8)
            sums_ref[half_at, pl.ds(at, size_at), :] = parts[side * PIECES + piece][...]

    def lanes_block(block):
        return jnp.concatenate([sums_ref[c, block * half:(block + 1) * half, :] for c in range(CORES)], axis=0)

    coefs = jnp.concatenate([lanes_block(b) for b in range(basis // LANES)], axis=1)
    own = jnp.concatenate([lanes_block(basis // LANES + b) for b in range(columns // LANES)], axis=1)
    row_at = lax.broadcasted_iota(jnp.int32, (columns, columns), 0)
    lane_at = lax.broadcasted_iota(jnp.int32, (columns, columns), 1)
    work_ref[:, :columns] = own - lax.dot_general(
        coefs, coefs, NT, precision=lax.Precision.HIGHEST, preferred_element_type=jnp.float32
    )
    work_ref[:, columns:] = (row_at == lane_at).astype(jnp.float32)
    coefs_s = split(coefs)
    leaf_count = rows // LEAF

    def project(leaf):
        span = slice(leaf * LEAF, (leaf + 1) * LEAF)
        block = yt_ref[:, :, span].reshape(columns, LEAF).T
        p_ref[span, :] = block - dot3(split(q_ref[span, :]), coefs_s, NT)

    uppers = []
    for k in range(rounds):
        here = slice(k * size, (k + 1) * size)
        after = slice((k + 1) * size, columns)
        if k > 0:
            for leaf in range((k - 1) * leaf_count // (rounds - 1), k * leaf_count // (rounds - 1)):
                project(leaf)
        upper, inverse = factor_block(work_ref[here, here])
        uppers.append(upper)
        done = dot4(split(inverse), split(work_ref[here, :]), NN)
        work_ref[here, :] = done
        if k + 1 < rounds:
            work_ref[after, :] -= dot4(split(done[:, after]), split(done), TN)
        if k == 0:
            q_copy.wait()
            y_copy.wait()
    zero = jnp.zeros((size, size), jnp.float32)
    diagonal = jnp.concatenate(
        [jnp.concatenate([uppers[k] if j == k else zero for j in range(rounds)], axis=1) for k in range(rounds)], axis=0
    )
    inverse = work_ref[:, columns:]
    inverse_t = split(jnp.where(row_at >= lane_at, inverse, 0.0))
    diagonal_s = split(diagonal)
    sums = []
    for leaf in range(leaf_count):
        span = slice(leaf * LEAF, (leaf + 1) * LEAF)
        fresh = dot3(split(p_ref[span, :]), inverse_t, NT)
        v_ref[span, :] = fresh
        remainder = dot3(split(fresh), diagonal_s, NN)
        sums.append(jnp.sum(remainder * remainder, axis=0, keepdims=True))
    count = len(sums)
    member = (
        lax.broadcasted_iota(jnp.int32, (8, columns), 0)
        == lax.broadcasted_iota(jnp.int32, (8, columns), 1) // size
    ).astype(jnp.float32)
    leaf_sums = jnp.concatenate(sums + [jnp.zeros((8 - count, columns), jnp.float32)], axis=0)
    leaf_energy = dot4(split(member), split(leaf_sums), NT)
    energies = jnp.sum(jnp.where(row_at == lane_at, own, 0.0), axis=0, keepdims=True)
    energy = jnp.sum(member * energies, axis=1, keepdims=True)
    est_ref[...] = jnp.sqrt(leaves * leaf_energy / energy)[:rounds, :count]


def run_finish(leaves, core, near, parts, prior_basis, samples_t):
    rows, basis = prior_basis.shape
    rounds, size, _ = samples_t.shape
    columns = rounds * size
    depth = (basis + columns) // LANES * (columns // CORES)
    whole = pl.BlockSpec(memory_space=pltpu.VMEM)
    held = [pltpu.with_memory_space_constraint(part, pltpu.VMEM) for part in parts]
    return pl.pallas_call(
        functools.partial(finish_kernel, leaves),
        in_specs=[pl.BlockSpec(memory_space=pltpu.SMEM)] * 2
        + [whole] * len(parts)
        + [pl.BlockSpec(memory_space=pl.ANY), pl.BlockSpec(memory_space=pl.ANY)],
        out_specs=[whole, whole],
        out_shape=[
            jax.ShapeDtypeStruct((rows, columns), jnp.float32),
            jax.ShapeDtypeStruct((rounds, rows // LEAF), jnp.float32),
        ],
        scratch_shapes=[
            pltpu.VMEM((rows, basis), jnp.float32),
            pltpu.VMEM((rounds, size, rows), jnp.float32),
            pltpu.VMEM((columns, 2 * columns), jnp.float32),
            pltpu.VMEM((rows, columns), jnp.float32),
            pltpu.VMEM((CORES, depth, LANES), jnp.float32),
            pltpu.SemaphoreType.DMA((2,)),
        ],
        name="finish",
    )(core, near, *held, prior_basis, samples_t)


def shifted(x, hops):
    count = lax.axis_size(CHIP)
    return lax.ppermute(x, CHIP, [(i, (i + hops) % count) for i in range(count)])


def local(prior_basis, samples):
    rounds, rows, size = samples.shape
    basis = prior_basis.shape[1]
    columns = rounds * size
    half = columns // CORES
    depth = (basis + columns) // LANES * half
    quarter = depth // NEAR
    far = lax.axis_size("far")
    core = lax.axis_index("core").reshape(1).astype(jnp.int32)
    near = lax.axis_index("near").reshape(1).astype(jnp.int32)
    step = LEAF
    samples_t = jnp.transpose(samples, (0, 2, 1))
    mine, theirs = pl.pallas_call(
        stats_kernel,
        grid=(rows // step,),
        in_specs=[
            pl.BlockSpec(memory_space=pltpu.SMEM),
            pl.BlockSpec(memory_space=pltpu.SMEM),
            pl.BlockSpec((step, basis), lambda i: (i, 0)),
            pl.BlockSpec((rounds, size, step), lambda i: (0, 0, i)),
        ],
        out_specs=[
            pl.BlockSpec(memory_space=pltpu.VMEM),
            pl.BlockSpec(memory_space=pltpu.VMEM),
        ],
        out_shape=[pltpu.VMEM((depth, LANES), jnp.float32), pltpu.VMEM((depth, LANES), jnp.float32)],
        scratch_shapes=[pltpu.VMEM((CORES, depth, LANES), jnp.float32)],
        name="stats",
    )(core, near, prior_basis, samples_t)
    chip = (mine + lax.ppermute(theirs, "core", SWAP)).reshape(NEAR, quarter, LANES)
    middle = quarter // 2
    from_left = shifted(chip[1], 1)
    from_right = shifted(chip[3], -1)
    from_far_left = shifted(chip[2, :middle], 2)
    from_far_right = shifted(chip[2, middle:], -2)
    near_sum = chip[0] + from_left + from_right + jnp.concatenate([from_far_left, from_far_right], axis=0)
    far_parts = lax.all_to_all(near_sum.reshape(far, quarter // far, LANES), "far", 0, 0, tiled=True)
    total = jnp.sum(far_parts, axis=0)
    own = lax.all_to_all(jnp.broadcast_to(total, far_parts.shape), "far", 0, 0, tiled=True).reshape(quarter, LANES)
    pieces = [own, shifted(own, -1), shifted(own, 1), shifted(own[:middle], 2), shifted(own[middle:], -2)]
    parts = pieces + [lax.ppermute(piece, "core", SWAP) for piece in pieces]
    leaves = float(rows // LEAF * far * NEAR * CORES)
    return run_finish(leaves, core, near, parts, prior_basis, samples_t)


def solution(mesh):
    grp = mesh.shape["grp"]
    far = mesh.shape["row"] // (NEAR * CORES)
    parts = Mesh(mesh.devices.reshape(grp, far, NEAR, CORES), GRP_ROW)
    in_specs = (P(GRP_ROW, None), P(None, GRP_ROW, None))
    out_specs = (P(GRP_ROW, None), P(None, GRP_ROW))
    return jax.shard_map(local, mesh=parts, in_specs=in_specs, out_specs=out_specs, check_vma=False)
```

```python
import functools

import jax
import jax.numpy as jnp
from jax import lax
from jax.experimental import pallas as pl
from jax.experimental.pallas import tpu as pltpu
from jax.sharding import Mesh
from jax.sharding import PartitionSpec as P

LEAF = 256
LANES = 128
NEAR = 4
CORES = 2
PIECES = 4
ROW = ("far", "near", "core")
GRP_ROW = ("grp",) + ROW
SWAP = [(0, 1), (1, 0)]
NT = (((1,), (1,)), ((), ()))
TN = (((0,), (0,)), ((), ()))
NN = (((1,), (0,)), ((), ()))


def split(x):
    high = x.astype(jnp.bfloat16)
    low = (x - high.astype(jnp.float32)).astype(jnp.bfloat16)
    return high, low


def dot_parts(a, b, dims, pairs):
    ((lhs_at,), (rhs_at,)), _ = dims
    lhs = jnp.concatenate([a[i] for i, _ in pairs], axis=lhs_at)
    rhs = jnp.concatenate([b[j] for _, j in pairs], axis=rhs_at)
    return lax.dot_general(lhs, rhs, dims, preferred_element_type=jnp.float32)


def dot3(a, b, dims):
    return dot_parts(a, b, dims, ((0, 0), (0, 1), (1, 0)))


def dot4(a, b, dims):
    return dot_parts(a, b, dims, ((0, 0), (0, 1), (1, 0), (1, 1)))


def stats_kernel(core_ref, near_ref, q_ref, yt_ref, mine_ref, theirs_ref, acc_ref):
    step = pl.program_id(0)
    yt = yt_ref[...].reshape(-1, yt_ref.shape[2])
    basis = q_ref.shape[1]
    half = yt.shape[0] // CORES
    quarter = acc_ref.shape[1] // NEAR
    ys = split(yt)
    with_basis = dot3(ys, split(q_ref[...]), NN)
    with_self = dot4(ys, ys, NT)

    @pl.when(step == 0)
    def _():
        acc_ref[...] = jnp.zeros_like(acc_ref)

    for c in range(CORES):
        rows = slice(c * half, (c + 1) * half)
        for product, base in ((with_basis, 0), (with_self, basis // LANES)):
            for block in range(product.shape[1] // LANES):
                at = (base + block) * half
                acc_ref[c, at:at + half, :] += product[rows, block * LANES:(block + 1) * LANES]

    @pl.when(step == pl.num_programs(0) - 1)
    def _():
        core, near = core_ref[0], near_ref[0]
        for out_ref, at in ((mine_ref, core), (theirs_ref, 1 - core)):
            for place, slot in enumerate(sent_slots(at)):
                source = pl.multiple_of(lax.rem(near + slot, NEAR) * quarter, 8)
                out_ref[place * quarter:(place + 1) * quarter, :] = acc_ref[at, pl.ds(source, quarter), :]


def sent_slots(core):
    return 0, 1 + 2 * core, 2, 3 - 2 * core


def received_slots(core):
    return 0, 3 - 2 * core, 2, 1 + 2 * core


def spread_row(x, r):
    return jnp.broadcast_to(x[r:r + 1], x.shape)


def factor_block(block, panel=8):
    size = block.shape[0]
    row_at = lax.broadcasted_iota(jnp.int32, (size, size), 0)
    lane_at = lax.broadcasted_iota(jnp.int32, (size, size), 1)
    eye = (row_at == lane_at).astype(jnp.float32)
    work = jnp.concatenate([block, eye], axis=1)
    width = 2 * size
    count = size // 8
    high = panel // 8
    parts = [work[8 * i:8 * i + 8] for i in range(count)]
    sub = lax.broadcasted_iota(jnp.int32, (8, width), 0)
    done = []
    for p in range(0, count, high):
        cols = {
            i: [jnp.take_along_axis(parts[i], jnp.full((8, width), 8 * p + m, jnp.int32), axis=1) for m in range(panel)]
            for i in range(p, count)
        }
        steps = []
        for q in range(p, p + high):
            pivots = None
            for r in range(0, 8, 2):
                m = 8 * (q - p) + r
                left, right = cols[q][m], cols[q][m + 1]
                a, b, c = spread_row(left, r), spread_row(right, r), spread_row(right, r + 1)
                determinant = a * c - b * b
                inverse = 1.0 / determinant
                ratio = 1.0 / a
                second = determinant * ratio
                pivots = a if r == 0 else jnp.where(sub == r, a, pivots)
                pivots = jnp.where(sub == r + 1, second, pivots)

                def adjugate(x):
                    x0, x1 = spread_row(x, r), spread_row(x, r + 1)
                    return c * x0 - b * x1, a * x1 - b * x0

                row0, row1 = adjugate(parts[q])
                heads = {k: adjugate(cols[q][k]) for k in range(m + 2, panel)}
                fixed = spread_row(parts[q], r + 1) - (b * ratio) * spread_row(parts[q], r)
                for i in range(q, p + high):
                    x0, x1 = cols[i][m], cols[i][m + 1]
                    if i == q:
                        x0, x1 = jnp.where(sub > r + 1, x0, 0.0), jnp.where(sub > r + 1, x1, 0.0)
                    for k, (head0, head1) in heads.items():
                        cols[i][k] = cols[i][k] - (x0 * head0 + x1 * head1) * inverse
                    parts[i] = parts[i] - (x0 * row0 + x1 * row1) * inverse
                parts[q] = jnp.where(sub == r + 1, fixed, parts[q])
                steps.append((m, row0 * inverse, row1 * inverse, {k: (h0 * inverse, h1 * inverse) for k, (h0, h1) in heads.items()}))
            done.append(parts[q] * lax.rsqrt(pivots))
        for i in range(p + high, count):
            col = cols[i]
            for m, row0, row1, heads in steps:
                parts[i] = parts[i] - (col[m] * row0 + col[m + 1] * row1)
                for k, (head0, head1) in heads.items():
                    col[k] = col[k] - (col[m] * head0 + col[m + 1] * head1)
    done = jnp.concatenate(done, axis=0)
    upper = jnp.where(row_at <= lane_at, done[:, :size], 0.0)
    return upper, done[:, size:]


def finish_kernel(leaves, core_ref, near_ref, *refs):
    parts = refs[:CORES * PIECES]
    q_hbm, yt_hbm, v_ref, est_ref, q_ref, yt_ref, work_ref, p_ref, sums_ref, sems = refs[CORES * PIECES:]
    q_copy = pltpu.make_async_copy(q_hbm, q_ref, sems.at[0])
    y_copy = pltpu.make_async_copy(yt_hbm, yt_ref, sems.at[1])
    q_copy.start()
    y_copy.start()
    rows, basis = q_ref.shape
    columns = yt_ref.shape[0] * yt_ref.shape[1]
    rounds = est_ref.shape[0]
    size = columns // rounds
    half = columns // CORES

    quarter = sums_ref.shape[1] // NEAR
    core, near = core_ref[0], near_ref[0]
    for side in range(CORES):
        half_at = core if side == 0 else 1 - core
        for piece, slot in enumerate(received_slots(half_at)):
            at = pl.multiple_of(lax.rem(near + slot, NEAR) * quarter, 8)
            sums_ref[half_at, pl.ds(at, quarter), :] = parts[side * PIECES + piece][...]

    def lanes_block(block):
        return jnp.concatenate([sums_ref[c, block * half:(block + 1) * half, :] for c in range(CORES)], axis=0)

    coefs = jnp.concatenate([lanes_block(b) for b in range(basis // LANES)], axis=1)
    own = jnp.concatenate([lanes_block(basis // LANES + b) for b in range(columns // LANES)], axis=1)
    row_at = lax.broadcasted_iota(jnp.int32, (columns, columns), 0)
    lane_at = lax.broadcasted_iota(jnp.int32, (columns, columns), 1)
    gram = own - lax.dot_general(coefs, coefs, NT, precision=lax.Precision.HIGHEST, preferred_element_type=jnp.float32)
    own_diagonal = jnp.where(row_at == lane_at, own, 0.0)
    energies = jnp.sum(own_diagonal, axis=0, keepdims=True)
    scale = lax.rsqrt(energies)
    scale_down = lax.rsqrt(jnp.sum(own_diagonal, axis=1, keepdims=True))
    work_ref[:, :columns] = gram * (scale * scale_down)
    work_ref[:, columns:] = jnp.where(row_at == lane_at, scale, 0.0)
    coefs_s = split(coefs)
    leaf_count = rows // LEAF

    def project(leaf):
        span = slice(leaf * LEAF, (leaf + 1) * LEAF)
        block = yt_ref[:, :, span].reshape(columns, LEAF).T
        p_ref[span, :] = block - dot3(split(q_ref[span, :]), coefs_s, NT)

    uppers = []
    for k in range(rounds):
        here = slice(k * size, (k + 1) * size)
        after = slice((k + 1) * size, columns)
        if k > 0:
            for leaf in range((k - 1) * leaf_count // (rounds - 1), k * leaf_count // (rounds - 1)):
                project(leaf)
        upper, inverse = factor_block(work_ref[here, here])
        uppers.append(upper)
        done = dot4(split(inverse), split(work_ref[here, :]), NN)
        work_ref[here, :] = done
        if k + 1 < rounds:
            work_ref[after, :] -= dot4(split(done[:, after]), split(done), TN)
        if k == 0:
            q_copy.wait()
            y_copy.wait()
    zero = jnp.zeros((size, size), jnp.float32)
    diagonal = jnp.concatenate(
        [jnp.concatenate([uppers[k] if j == k else zero for j in range(rounds)], axis=1) for k in range(rounds)], axis=0
    )
    diagonal = diagonal * (energies * scale)
    inverse = work_ref[:, columns:]
    inverse_t = split(jnp.where(row_at >= lane_at, inverse, 0.0))
    diagonal_s = split(diagonal)
    sums = []
    for leaf in range(leaf_count):
        span = slice(leaf * LEAF, (leaf + 1) * LEAF)
        fresh = dot3(split(p_ref[span, :]), inverse_t, NT)
        v_ref[span, :] = fresh
        remainder = dot3(split(fresh), diagonal_s, NN)
        sums.append(jnp.sum(remainder * remainder, axis=0, keepdims=True))
    count = len(sums)
    member = (
        lax.broadcasted_iota(jnp.int32, (8, columns), 0)
        == lax.broadcasted_iota(jnp.int32, (8, columns), 1) // size
    ).astype(jnp.float32)
    leaf_sums = jnp.concatenate(sums + [jnp.zeros((8 - count, columns), jnp.float32)], axis=0)
    leaf_energy = dot4(split(member), split(leaf_sums), NT)
    energy = jnp.sum(member * energies, axis=1, keepdims=True)
    est_ref[...] = jnp.sqrt(leaves * leaf_energy / energy)[:rounds, :count]


def run_finish(leaves, core, near, parts, prior_basis, samples_t):
    rows, basis = prior_basis.shape
    rounds, size, _ = samples_t.shape
    columns = rounds * size
    depth = (basis + columns) // LANES * (columns // CORES)
    whole = pl.BlockSpec(memory_space=pltpu.VMEM)
    held = [pltpu.with_memory_space_constraint(part, pltpu.VMEM) for part in parts]
    return pl.pallas_call(
        functools.partial(finish_kernel, leaves),
        in_specs=[pl.BlockSpec(memory_space=pltpu.SMEM)] * 2
        + [whole] * len(parts)
        + [pl.BlockSpec(memory_space=pl.ANY), pl.BlockSpec(memory_space=pl.ANY)],
        out_specs=[whole, whole],
        out_shape=[
            jax.ShapeDtypeStruct((rows, columns), jnp.float32),
            jax.ShapeDtypeStruct((rounds, rows // LEAF), jnp.float32),
        ],
        scratch_shapes=[
            pltpu.VMEM((rows, basis), jnp.float32),
            pltpu.VMEM((rounds, size, rows), jnp.float32),
            pltpu.VMEM((columns, 2 * columns), jnp.float32),
            pltpu.VMEM((rows, columns), jnp.float32),
            pltpu.VMEM((CORES, depth, LANES), jnp.float32),
            pltpu.SemaphoreType.DMA((2,)),
        ],
        name="finish",
    )(core, near, *held, prior_basis, samples_t)


def shifted(x, hops):
    chips = lax.axis_size("far") * NEAR
    pairs = []
    for chip in range(chips):
        pairs.append((chip * CORES, (chip + hops) % chips * CORES))
        pairs.append((chip * CORES + 1, (chip - hops) % chips * CORES + 1))
    return lax.ppermute(x, ROW, pairs)


def local(prior_basis, samples):
    rounds, rows, size = samples.shape
    basis = prior_basis.shape[1]
    columns = rounds * size
    half = columns // CORES
    depth = (basis + columns) // LANES * half
    quarter = depth // NEAR
    far = lax.axis_size("far")
    core = lax.axis_index("core").reshape(1).astype(jnp.int32)
    near = lax.axis_index("near").reshape(1).astype(jnp.int32)
    step = LEAF
    samples_t = jnp.transpose(samples, (0, 2, 1))
    mine, theirs = pl.pallas_call(
        stats_kernel,
        grid=(rows // step,),
        in_specs=[
            pl.BlockSpec(memory_space=pltpu.SMEM),
            pl.BlockSpec(memory_space=pltpu.SMEM),
            pl.BlockSpec((step, basis), lambda i: (i, 0)),
            pl.BlockSpec((rounds, size, step), lambda i: (0, 0, i)),
        ],
        out_specs=[
            pl.BlockSpec(memory_space=pltpu.VMEM),
            pl.BlockSpec(memory_space=pltpu.VMEM),
        ],
        out_shape=[pltpu.VMEM((depth, LANES), jnp.float32), pltpu.VMEM((depth, LANES), jnp.float32)],
        scratch_shapes=[pltpu.VMEM((CORES, depth, LANES), jnp.float32)],
        name="stats",
    )(core, near, prior_basis, samples_t)
    chip = (mine + lax.ppermute(theirs, "core", SWAP)).reshape(NEAR, quarter, LANES)
    two_on = shifted(chip[2], 2)
    one_on = shifted(chip[1], 1)
    one_back = shifted(chip[3], -1)
    near_sum = chip[0] + one_on + one_back + two_on
    far_parts = lax.all_to_all(near_sum.reshape(far, quarter // far, LANES), "far", 0, 0, tiled=True)
    total = jnp.sum(far_parts, axis=0)
    own = lax.all_to_all(jnp.broadcast_to(total, far_parts.shape), "far", 0, 0, tiled=True).reshape(quarter, LANES)
    pieces = [own, shifted(own, 1), shifted(own, 2), shifted(own, -1)]
    parts = pieces + [lax.ppermute(piece, "core", SWAP) for piece in pieces]
    leaves = float(rows // LEAF * far * NEAR * CORES)
    return run_finish(leaves, core, near, parts, prior_basis, samples_t)


def solution(mesh):
    grp = mesh.shape["grp"]
    far = mesh.shape["row"] // (NEAR * CORES)
    parts = Mesh(mesh.devices.reshape(grp, far, NEAR, CORES), GRP_ROW)
    in_specs = (P(GRP_ROW, None), P(None, GRP_ROW, None))
    out_specs = (P(GRP_ROW, None), P(None, GRP_ROW))
    return jax.shard_map(local, mesh=parts, in_specs=in_specs, out_specs=out_specs, check_vma=False)
```
